32 devices in a mesh: dp: 2 (over y), fsdp: 16 (over z, x, core).
Axes of the slice: x: 2, y: 2, z: 4, core: 2. Of those that a mesh axis runs over, the one named last changes fastest.
Arguments:
- tokens: bfloat16 [12288, 1024], P(('dp', 'fsdp')), may hold values from -6.5 to 6.5
- cotangent: bfloat16 [12288, 1024], P(('dp', 'fsdp')), may hold values from -6 to 6
- patch_count: int32 [32], P(('dp', 'fsdp')), may hold values from 96 to 384, as said below
- image_starts: int32 [32, 8], P(('dp', 'fsdp')), may hold values from 0 to 384, as said below
- qkv_weight: bfloat16 [1024, 3072], P('fsdp'), may hold values from -8 to 8
- proj_weight: bfloat16 [1024, 1024], P('fsdp'), may hold values from -0.1875 to 0.1875
- norm_gain: bfloat16 [1024], P('fsdp'), may hold values from 0.25 to 1.75
- norm_shift: bfloat16 [1024], P('fsdp'), may hold values from -3 to 3
Outputs:
- grad_tokens: bfloat16 [12288, 1024], P(('dp', 'fsdp'))
- qkv_grad: float32 [1024, 3072], P('fsdp')
- proj_grad: float32 [1024, 1024], P('fsdp')
- gain_grad: float32 [1024], P('fsdp')
- shift_grad: float32 [1024], P('fsdp')
The draws below stay inside these ranges and needn't reach their ends.
Inputs may be any that keep to these rules, and one draw needn't show every extreme that they name: `patch_count`: at least one device has all 384 slots live; live slots of a device come first. `image_starts`: per device, non-decreasing and first 0; an image runs from its start to the next start or to the device's patch count; a start equal to the patch count marks an absent image; no image has more than 192 patches.
All inputs are finite; a program needn't handle non-finite values.
Results may differ from the reference program's by a relative error of at most 0.025.
The reference program's roundings to bfloat16 on the way count: a program that leaves them out, or rounds other values in their place, can miss the bound.
Values may be sent and summed in bfloat16 or wider, within the bound.
No kernel may reach another device: no remote copies, remote signals or barrier semaphores. Data moves between devices by JAX's collectives and lax.ppermute only.
A program may use at most 128 MiB of HBM per device.

```python
import math
import jax
import jax.numpy as jnp
from jax import lax

D = 1024
HEAD_DIM = 64
HEADS = 16
TOK_DEV = 384
IMG_DEV = 8
TOKENS = 12288
N_DP = 2
N_FSDP = 16


def layout_draw(key):
    devices_all = N_DP * N_FSDP
    lengths = jax.random.randint(jax.random.fold_in(key, 11), (devices_all, IMG_DEV), TOK_DEV // 16 + 1, TOK_DEV // 2 + 1)
    limits = jax.random.randint(jax.random.fold_in(key, 12), (devices_all,), TOK_DEV // 4, TOK_DEV + 1)
    chosen = jax.random.randint(jax.random.fold_in(key, 13), (), 0, devices_all)
    picked = jnp.arange(devices_all, dtype=jnp.int32) == chosen
    limits = jnp.where(picked, TOK_DEV, limits)
    lengths = jnp.where(picked[:, None], TOK_DEV // 2, lengths)
    ends = jnp.cumsum(lengths, axis=1)
    starts = ends - lengths
    counts = jnp.minimum(ends[:, -1], limits).astype(jnp.int32)
    starts = jnp.minimum(starts, counts[:, None]).astype(jnp.int32)
    return (counts, starts)


def draw_patch_count(key, part):
    return layout_draw(key)[0]


def draw_image_starts(key, part):
    return layout_draw(key)[1]


def draw_tokens(key, part):
    base = jnp.clip(jax.random.normal(jax.random.fold_in(key, 21), (TOKENS, D), jnp.float32), -6.0, 6.0)
    return base.astype(jnp.bfloat16)


def draw_qkv_weight(key, part):
    base = jnp.clip(jax.random.normal(jax.random.fold_in(key, 31), (D, 3 * D), jnp.float32), -6.0, 6.0) * D ** (-0.5)
    return base.astype(jnp.bfloat16)


def block_scale(key, extent, cuts, least, top_value):
    factor_of, own = 1.0, jax.random.fold_in(key, 6)
    for axis_at, blocks in cuts:
        heights = jnp.exp(jax.random.uniform(jax.random.fold_in(own, axis_at), (blocks,), jnp.float32, least / len(cuts), top_value / len(cuts)))
        factor_of = factor_of * jnp.repeat(heights, extent[axis_at] // blocks).reshape([-1 if axis == axis_at else 1 for axis in range(len(extent))])
    return factor_of


def centred(own_key, extent, scale, limit, cuts=(), held_as=jnp.bfloat16):
    values = scale * jax.random.normal(own_key, extent, jnp.float32)
    if cuts:
        values = values * block_scale(own_key, extent, cuts, -0.22, 0.18)
    return jnp.clip(values, -limit, limit).astype(held_as)


def setup_inputs(seed: int = 0) -> dict:
    streams_of = jax.random.split(jax.random.key(seed), 9)
    return {
        "tokens": draw_tokens(jax.random.fold_in(streams_of[8], 71), 0),
        "cotangent": centred(streams_of[1], (TOKENS, D), 1.0, 6.0, ((0, 32),)),
        "patch_count": draw_patch_count(jax.random.fold_in(streams_of[8], 71), 0),
        "image_starts": draw_image_starts(jax.random.fold_in(streams_of[8], 71), 0),
        "qkv_weight": draw_qkv_weight(jax.random.fold_in(streams_of[8], 71), 0),
        "proj_weight": centred(streams_of[5], (D, D), D ** -0.5, 0.1875, ((0, 16),)),
        "norm_gain": jnp.clip(1.0 + 0.15 * jax.random.normal(streams_of[6], (D,), jnp.float32), 0.25, 1.75).astype(jnp.bfloat16),
        "norm_shift": centred(streams_of[7], (D,), 0.5, 3.0, ((0, 16),)),
    }


norm_eps = 1e-06
masked_score = -1e+30

def block_backward(block_tokens, block_cot, live_count, starts, qkv_weight, proj_weight, norm_gain, norm_shift):
    rows = block_tokens.shape[0]
    factor = HEAD_DIM ** (-0.5)
    position = jnp.arange(rows, dtype=jnp.int32)
    live = position < live_count
    segment = lax.optimization_barrier(jnp.sum((starts[None, :] <= position[:, None]).astype(jnp.int32), axis=1))
    allowed = live[:, None] & live[None, :] & (segment[:, None] == segment[None, :])
    source = block_tokens.astype(jnp.float32)
    center = lax.optimization_barrier(jnp.mean(source, axis=1, keepdims=True))
    centered = source - center
    variance = lax.optimization_barrier(jnp.mean(centered * centered, axis=1, keepdims=True))
    inverse = lax.rsqrt(variance + norm_eps)
    normed = centered * inverse
    gain = norm_gain.astype(jnp.float32)
    hidden = (normed * gain + norm_shift.astype(jnp.float32)).astype(jnp.bfloat16)
    qkv = jnp.dot(hidden, qkv_weight, preferred_element_type=jnp.float32).astype(jnp.bfloat16)
    split = qkv.reshape(rows, 3, HEADS, HEAD_DIM)
    queries = split[:, 0].astype(jnp.float32)
    keys = split[:, 1].astype(jnp.float32)
    values = split[:, 2].astype(jnp.float32)
    scores = jnp.einsum('qhe,khe->hqk', queries, keys) * factor
    scores = jnp.where(allowed[None], scores, masked_score)
    row_max = lax.optimization_barrier(jnp.max(scores, axis=2, keepdims=True))
    expon = jnp.exp(scores - row_max)
    probs = expon / lax.optimization_barrier(jnp.sum(expon, axis=2, keepdims=True))
    probs_low = probs.astype(jnp.bfloat16).astype(jnp.float32)
    attended = jnp.einsum('hqk,khe->qhe', probs_low, values).reshape(rows, D).astype(jnp.bfloat16)
    masked_cot = jnp.where(live[:, None], block_cot, jnp.zeros_like(block_cot))
    proj_term = jnp.dot(attended.T, masked_cot, preferred_element_type=jnp.float32)
    grad_attended = jnp.dot(masked_cot, proj_weight.T, preferred_element_type=jnp.float32).astype(jnp.bfloat16)
    grad_heads = grad_attended.reshape(rows, HEADS, HEAD_DIM).astype(jnp.float32)
    grad_probs = jnp.einsum('qhe,khe->hqk', grad_heads, values)
    grad_values = jnp.einsum('hqk,qhe->khe', probs_low, grad_heads).astype(jnp.bfloat16)
    grad_scores = probs * (grad_probs - lax.optimization_barrier(jnp.sum(probs * grad_probs, axis=2, keepdims=True))) * factor
    grad_scores = grad_scores.astype(jnp.bfloat16).astype(jnp.float32)
    grad_queries = jnp.einsum('hqk,khe->qhe', grad_scores, keys).astype(jnp.bfloat16)
    grad_keys = jnp.einsum('hqk,qhe->khe', grad_scores, queries).astype(jnp.bfloat16)
    grad_qkv = jnp.stack([grad_queries, grad_keys, grad_values], axis=1).reshape(rows, 3 * D)
    qkv_term = jnp.dot(hidden.T, grad_qkv, preferred_element_type=jnp.float32)
    grad_hidden = jnp.dot(grad_qkv, qkv_weight.T, preferred_element_type=jnp.float32)
    gain_term = lax.optimization_barrier(jnp.sum(grad_hidden * normed, axis=0))
    shift_term = lax.optimization_barrier(jnp.sum(grad_hidden, axis=0))
    grad_normed = grad_hidden * gain
    inner = grad_normed - lax.optimization_barrier(jnp.mean(grad_normed, axis=1, keepdims=True))
    inner = inner - normed * lax.optimization_barrier(jnp.mean(grad_normed * normed, axis=1, keepdims=True))
    grad_block = (block_cot.astype(jnp.float32) + inverse * inner).astype(jnp.bfloat16)
    return (grad_block, qkv_term, proj_term, gain_term, shift_term)

def reference(tokens, cotangent, patch_count, image_starts, qkv_weight, proj_weight, norm_gain, norm_shift):
    device_count = patch_count.shape[0]
    token_blocks = tokens.reshape(device_count, TOK_DEV, D)
    cot_blocks = cotangent.reshape(device_count, TOK_DEV, D)

    def visit(totals, inputs):
        block_tokens, block_cot, live_count, starts = inputs
        grad_block, qkv_term, proj_term, gain_term, shift_term = block_backward(block_tokens, block_cot, live_count, starts, qkv_weight, proj_weight, norm_gain, norm_shift)
        totals = (totals[0] + qkv_term, totals[1] + proj_term, totals[2] + gain_term, totals[3] + shift_term)
        return (totals, grad_block)
    start_totals = (jnp.zeros((D, 3 * D), jnp.float32), jnp.zeros((D, D), jnp.float32), jnp.zeros((D,), jnp.float32), jnp.zeros((D,), jnp.float32))
    totals, grad_blocks = lax.scan(visit, start_totals, (token_blocks, cot_blocks, patch_count, image_starts))
    factor = 1.0 / math.sqrt(TOKENS)
    return (grad_blocks.reshape(TOKENS, D), totals[0] * factor, totals[1] * factor, totals[2] * factor, totals[3] * factor)
```

```python
import math

import jax
import jax.numpy as jnp
from jax import lax
from jax.sharding import PartitionSpec as P

HEAD_DIM = 64
norm_eps = 1e-06
masked_score = -1e30
bf16 = jnp.bfloat16
f32 = jnp.float32


def ring_chips(chips):
    half = chips // 2
    if chips % 2:
        return list(range(chips))
    return [2 * i for i in range(half)] + [2 * i + 1 for i in reversed(range(half))]


def ring_place(chip, chips):
    if chips % 2:
        return chip
    return jnp.where(chip % 2 == 0, chip // 2, chips - 1 - chip // 2)


def ring_chip(place, chips):
    if chips % 2:
        return place
    half = chips // 2
    return jnp.where(place < half, 2 * place, 2 * (chips - 1 - place) + 1)


def ring_pairs(chips, step):
    order = ring_chips(chips)
    return [
        (2 * order[i] + c, 2 * order[(i + step) % chips] + c) for i in range(chips) for c in range(2)
    ]


def swap_cores(x):
    n = lax.axis_size("fsdp")
    return lax.ppermute(x, "fsdp", [(i, i ^ 1) for i in range(n)])


def swap_bit(x, axis, bit):
    n = lax.axis_size(axis)
    return lax.ppermute(x, axis, [(i, i ^ bit) for i in range(n)])


def small_sum(x, axes):
    for axis in axes:
        n = lax.axis_size(axis)
        if n & (n - 1):
            x = lax.psum(x, axis)
            continue
        bit = 1
        while bit < n:
            x = x + swap_bit(x, axis, bit)
            bit *= 2
    return x


def ring_gather(block, chips, place, step):
    pairs = ring_pairs(chips, step)
    whole = jnp.zeros((chips,) + block.shape, block.dtype)
    held = block
    for s in range(chips):
        at = ring_chip((place - step * s) % chips, chips)
        whole = lax.dynamic_update_slice(whole, held[None], (at, 0, 0))
        if s + 1 < chips:
            held = lax.ppermute(held, "fsdp", pairs)
    return whole


def ring_scatter(term, chips, place, step):
    pairs = ring_pairs(chips, step)

    def piece(s):
        at = ring_chip((place - step * s) % chips, chips)
        return lax.dynamic_index_in_dim(term, at, 0, keepdims=False)

    held = piece(1).astype(bf16)
    for s in range(2, chips + 1):
        got = lax.ppermute(held, "fsdp", pairs)
        held = (got.astype(f32) + piece(s).astype(f32)).astype(bf16)
    return held


def replica_sum(x):
    if lax.axis_size("dp") == 2:
        return x.astype(f32) + swap_bit(x, "dp", 1).astype(f32)
    return lax.psum(x, "dp").astype(f32)


def attention_grads(qkv, grad_heads, segment, heads):
    blocks, rows = segment.shape
    factor = HEAD_DIM ** (-0.5)
    split = qkv.reshape(blocks, rows, 3, heads, HEAD_DIM)
    queries, keys, values = split[:, :, 0], split[:, :, 1], split[:, :, 2]
    allowed = segment[:, :, None] == segment[:, None, :]
    dot = lambda s, a, b: jnp.einsum(s, a, b, preferred_element_type=f32)
    scores = dot("bqhe,bkhe->bhqk", queries, keys) * factor
    scores = jnp.where(allowed[:, None], scores, masked_score)
    expon = jnp.exp(scores - jnp.max(scores, axis=3, keepdims=True))
    probs = expon / jnp.sum(expon, axis=3, keepdims=True)
    low = probs.astype(bf16)
    attended = dot("bhqk,bkhe->bqhe", low, values).astype(bf16)
    gh = grad_heads.reshape(blocks, rows, heads, HEAD_DIM)
    grad_probs = dot("bqhe,bkhe->bhqk", gh, values)
    grad_values = dot("bhqk,bqhe->bkhe", low, gh).astype(bf16)
    gs = probs * (grad_probs - jnp.sum(probs * grad_probs, axis=3, keepdims=True)) * factor
    gs = gs.astype(bf16)
    grad_queries = dot("bhqk,bkhe->bqhe", gs, keys).astype(bf16)
    grad_keys = dot("bhqk,bqhe->bkhe", gs, queries).astype(bf16)
    grad_qkv = jnp.stack([grad_queries, grad_keys, grad_values], axis=2)
    return (
        attended.reshape(blocks * rows, heads * HEAD_DIM),
        grad_qkv.reshape(blocks * rows, 3 * heads * HEAD_DIM),
    )


def per_device(
    tokens, cotangent, patch_count, image_starts, qkv_weight, proj_weight, norm_gain, norm_shift
):
    rows, d = tokens.shape
    own_rows = qkv_weight.shape[0]
    owners = lax.axis_size("fsdp")
    replicas = lax.axis_size("dp")
    chips = owners // 2
    me = lax.axis_index("fsdp")
    chip, core = me // 2, me % 2
    place = ring_place(chip, chips)
    even = core == 0
    heads = d // HEAD_DIM // 2
    width = 3 * heads * HEAD_DIM
    pairs_cols = heads * HEAD_DIM

    vec = jnp.zeros((2, owners, own_rows), bf16)
    vec = lax.dynamic_update_slice(
        vec, jnp.stack([norm_gain, norm_shift])[:, None], (0, me, 0)
    )
    vec = small_sum(vec.reshape(2, d), ("fsdp",))
    gain = vec[0].astype(f32)
    shift = vec[1].astype(f32)

    parts = qkv_weight.reshape(own_rows, 3 * heads, 2, HEAD_DIM)
    first, second = parts[:, :, 0].reshape(own_rows, width), parts[:, :, 1].reshape(own_rows, width)
    mine, others = jnp.where(even, first, second), jnp.where(even, second, first)
    got = swap_cores(others)
    block = jnp.where(
        even, jnp.concatenate([mine, got], axis=0), jnp.concatenate([got, mine], axis=0)
    )
    w_cw = ring_gather(block[:, : width // 2], chips, place, 1).reshape(d, width // 2)
    w_ccw = ring_gather(block[:, width // 2 :], chips, place, -1).reshape(d, width // 2)
    if own_rows == HEAD_DIM:
        p_cw = ring_gather(proj_weight[:, : d // 2], chips, place, 1).reshape(pairs_cols, d // 2)
        p_ccw = ring_gather(proj_weight[:, d // 2 :], chips, place, -1).reshape(pairs_cols, d // 2)
        proj = jnp.concatenate([p_cw, p_ccw], axis=1)
    else:
        proj = lax.all_gather(proj_weight, "fsdp", axis=0, tiled=True)
        proj = proj.reshape(heads, 2, HEAD_DIM, d)
        proj = jnp.where(even, proj[:, 0], proj[:, 1]).reshape(pairs_cols, d)

    position = jnp.arange(rows, dtype=jnp.int32)
    live = position < patch_count[0]
    segment = jnp.sum((image_starts[0][None, :] <= position[:, None]).astype(jnp.int32), axis=1)
    segment = jnp.where(live, segment, image_starts.shape[1] + 1)
    masked_cot = jnp.where(live[:, None], cotangent, jnp.zeros_like(cotangent))

    source = tokens.astype(f32)
    centered = source - jnp.mean(source, axis=1, keepdims=True)
    variance = jnp.mean(centered * centered, axis=1, keepdims=True)
    inverse = lax.rsqrt(variance + norm_eps)
    normed = centered * inverse
    hidden = (normed * gain + shift).astype(bf16)

    segments = jnp.stack([segment, swap_cores(segment)])
    hiddens = jnp.concatenate([hidden, swap_cores(hidden)], axis=0)
    cots = jnp.concatenate([masked_cot, swap_cores(masked_cot)], axis=0)

    dot = lambda a, b, dims: lax.dot_general(a, b, (dims, ((), ())), preferred_element_type=f32)
    weight = jnp.concatenate([w_cw, w_ccw], axis=1)
    qkv = dot(hiddens, weight, ((1,), (0,))).astype(bf16)
    grad_att = dot(cots, proj, ((1,), (1,))).astype(bf16)
    attended, grad_qkv = attention_grads(qkv, grad_att, segments, heads)

    proj_term = dot(attended, cots, ((0,), (0,))).astype(bf16).reshape(heads, HEAD_DIM, d)
    qkv_term = dot(hiddens, grad_qkv, ((0,), (0,))).astype(bf16).reshape(chips, d // chips, width)

    q_cw = ring_scatter(qkv_term[:, :, : width // 2], chips, place, 1)
    q_ccw = ring_scatter(qkv_term[:, :, width // 2 :], chips, place, -1)
    if own_rows == HEAD_DIM:
        o_cw = ring_scatter(proj_term[:, :, : d // 2], chips, place, 1)
        o_ccw = ring_scatter(proj_term[:, :, d // 2 :], chips, place, -1)
        o_sum = jnp.concatenate([o_cw, o_ccw], axis=1)
    else:
        none = jnp.zeros_like(proj_term)
        spread = jnp.stack(
            [jnp.where(even, proj_term, none), jnp.where(even, none, proj_term)], axis=1
        )
        o_sum = lax.psum_scatter(spread.reshape(d, d), "fsdp", scatter_dimension=0, tiled=True)

    grad_hidden = dot(grad_qkv, weight, ((1,), (1,)))
    grad_hidden = grad_hidden[:rows] + swap_cores(grad_hidden[rows:].astype(bf16)).astype(f32)
    vec_term = jnp.stack([jnp.sum(grad_hidden * normed, axis=0), jnp.sum(grad_hidden, axis=0)])
    grad_normed = grad_hidden * gain
    inner = grad_normed - jnp.mean(grad_normed, axis=1, keepdims=True)
    inner = inner - normed * jnp.mean(grad_normed * normed, axis=1, keepdims=True)
    grad_block = (cotangent.astype(f32) + inverse * inner).astype(bf16)

    scale = 1.0 / math.sqrt(rows * replicas * owners)
    proj_grad = replica_sum(o_sum) * scale
    q_sum = jnp.concatenate([q_cw, q_ccw], axis=1)
    low, high = q_sum[:own_rows], q_sum[own_rows:]
    keep, give = jnp.where(even, low, high), jnp.where(even, high, low)
    got = swap_cores(give)
    pair = jnp.stack([jnp.where(even, keep, got), jnp.where(even, got, keep)])
    pair = pair.reshape(2, own_rows, 3 * heads, HEAD_DIM).transpose(1, 2, 0, 3)
    qkv_grad = replica_sum(pair.reshape(own_rows, 2 * width)) * scale
    vec_sum = small_sum(vec_term, ("fsdp", "dp")) * scale
    vec_own = lax.dynamic_slice(vec_sum, (0, me * own_rows), (2, own_rows))
    return grad_block, qkv_grad, proj_grad, vec_own[0], vec_own[1]


def solution(mesh):
    both = P(("dp", "fsdp"))
    rows2 = P(("dp", "fsdp"), None)
    own2, own = P("fsdp", None), P("fsdp")
    return jax.shard_map(
        per_device,
        mesh=mesh,
        in_specs=(rows2, rows2, both, rows2, own2, own2, own, own),
        out_specs=(rows2, own2, own2, own, own),
        check_vma=False,
    )
```

```python
import functools
import math

import jax
import jax.numpy as jnp
from jax import lax
from jax.experimental import pallas as pl
from jax.experimental.pallas import tpu as pltpu
from jax.sharding import PartitionSpec as P

HEAD_DIM = 64
norm_eps = 1e-06
masked_score = -1e30
bf16 = jnp.bfloat16
f32 = jnp.float32


def ring_chips(chips):
    if chips % 2:
        return list(range(chips))
    half = chips // 2
    return [2 * i for i in range(half)] + [2 * i + 1 for i in reversed(range(half))]


def ring_place(chip, chips):
    if chips % 2:
        return chip
    return jnp.where(chip % 2 == 0, chip // 2, chips - 1 - chip // 2)


def ring_chip(place, chips):
    if chips % 2:
        return place
    return jnp.where(place < chips // 2, 2 * place, 2 * (chips - 1 - place) + 1)


def ring_step(x, chips, step):
    order = ring_chips(chips)
    pairs = [
        (2 * order[i] + c, 2 * order[(i + step) % chips] + c) for i in range(chips) for c in range(2)
    ]
    return lax.ppermute(x, "fsdp", pairs)


def swap_bit(x, axis, bit):
    n = lax.axis_size(axis)
    return lax.ppermute(x, axis, [(i, i ^ bit) for i in range(n)])


def swap_cores(x):
    return swap_bit(x, "fsdp", 1)


def small_sum(x, axes):
    for axis in axes:
        n = lax.axis_size(axis)
        if n & (n - 1):
            x = lax.psum(x, axis)
            continue
        bit = 1
        while bit < n:
            x = x + swap_bit(x, axis, bit)
            bit *= 2
    return x


def reach(chips, step, wide):
    far, near = chips // 2, chips - 1 - chips // 2
    return far if (step < 0) == wide else near


def offsets(chips, wide):
    ahead, behind = reach(chips, -1, wide), reach(chips, 1, wide)
    return [0] + [-(s + 1) for s in range(ahead)] + [s + 1 for s in range(behind)]


def ring_gather(block, chips, wide):
    pieces = [block]
    for step in (1, -1):
        held = block
        for _ in range(reach(chips, -step, wide)):
            held = ring_step(held, chips, step)
            pieces.append(held)
    return pieces


def ring_scatter(pieces, chips, wide):
    place_of = {o: i for i, o in enumerate(offsets(chips, wide))}
    total = pieces[0].astype(f32)
    for step in (1, -1):
        k = reach(chips, step, wide)
        held = pieces[place_of[step * k]]
        for t in range(1, k + 1):
            got = ring_step(held, chips, step)
            if t < k:
                own = pieces[place_of[step * (k - t)]]
                held = (got.astype(f32) + own.astype(f32)).astype(bf16)
        total = total + got.astype(f32)
    return total.astype(bf16)


def replica_sum(x):
    if lax.axis_size("dp") == 2:
        return x.astype(f32) + swap_bit(x, "dp", 1).astype(f32)
    return lax.psum(x, "dp").astype(f32)


def dot(a, b, contract):
    return lax.dot_general(a, b, (((contract[0],), (contract[1],)), ((), ())), preferred_element_type=f32)


def attention(qkv, grads, seg_col, seg_row, att, grad_qkv, rows, heads):
    width = heads * HEAD_DIM
    factor = HEAD_DIM ** (-0.5)
    lane = lax.broadcasted_iota(jnp.int32, (rows, 2 * HEAD_DIM), 1)

    def block(b, carry):
        at = pl.ds(b * rows, rows)
        allowed = seg_col[at, :] == seg_row[b]
        for pair in range(heads // 2):
            lanes = pl.ds(pair * 2 * HEAD_DIM, 2 * HEAD_DIM)
            q = qkv[at, lanes]
            k = qkv[at, pl.ds(width + pair * 2 * HEAD_DIM, 2 * HEAD_DIM)]
            v = qkv[at, pl.ds(2 * width + pair * 2 * HEAD_DIM, 2 * HEAD_DIM)]
            g = grads[at, lanes]
            sums = None
            for side in range(2):
                pick = (lane < HEAD_DIM) if side == 0 else (lane >= HEAD_DIM)
                only = lambda x: jnp.where(pick, x, jnp.zeros_like(x))
                qs, ks, vs, gs = only(q), only(k), only(v), only(g)
                scores = dot(qs, k, (1, 1)) * factor
                scores = jnp.where(allowed, scores, masked_score)
                expon = jnp.exp(scores - jnp.max(scores, axis=1, keepdims=True))
                probs = expon * (1.0 / jnp.sum(expon, axis=1, keepdims=True))
                low = probs.astype(bf16)
                grad_probs = dot(gs, v, (1, 1))
                moved = jnp.sum(probs * grad_probs, axis=1, keepdims=True)
                grad_scores = (probs * (grad_probs - moved) * factor).astype(bf16)
                new = (
                    dot(low, vs, (1, 0)),
                    dot(grad_scores, ks, (1, 0)),
                    dot(grad_scores, qs, (0, 0)),
                    dot(low, gs, (0, 0)),
                )
                sums = new if sums is None else tuple(x + y for x, y in zip(sums, new))
            att[at, lanes] = sums[0].astype(bf16)
            for i in range(3):
                to = pl.ds(i * width + pair * 2 * HEAD_DIM, 2 * HEAD_DIM)
                grad_qkv[at, to] = sums[i + 1].astype(bf16)
        return carry

    lax.fori_loop(0, seg_row.shape[0], block, 0)


def first_kernel(chips, rows, heads, fold, chip_of, seg_col, seg_row, tokens, cots, vec, *refs):
    pieces, refs = refs[:chips], refs[chips:]
    if fold:
        proj_in = None
    else:
        proj_in, refs = refs[0], refs[1:]
    hid, att, ghid, proj_rest, refs = *refs[:4], refs[4:]
    terms, refs = refs[:chips], refs[chips:]
    weight, proj, qkv, grads, grad_qkv, term = refs
    width = heads * HEAD_DIM
    tall = pieces[0].shape[0]
    half = 3 * width

    step = 64

    def norm(i, carry):
        at = pl.ds(i * step, step)
        source = tokens[at, :].astype(f32)
        centered = source - jnp.mean(source, axis=1, keepdims=True)
        variance = jnp.mean(centered * centered, axis=1, keepdims=True)
        normed = centered * lax.rsqrt(variance + norm_eps)
        hid[at, :] = (normed * vec[0:1, :] + vec[1:2, :]).astype(bf16)
        return carry

    lax.fori_loop(0, tokens.shape[0] // step, norm, 0)
    for j in range(chips):
        weight[pl.ds(chip_of[j] * tall, tall), :] = pieces[j][:, :half]
        if fold:
            low = tall // 2
            at = pl.ds(chip_of[j] * low, low)
            side = tokens.shape[1] // 2
            proj[at, :side] = pieces[j][:low, half:]
            proj[at, side:] = pieces[j][low:, half:]
    if not fold:
        proj[...] = proj_in[...]
    proj_rest[...] = proj[width:, :]
    qkv[...] = dot(hid[...], weight[...], (1, 0)).astype(bf16)
    grads[...] = dot(cots[...], proj[:width, :], (1, 1)).astype(bf16)
    attention(qkv, grads, seg_col, seg_row, att, grad_qkv, rows, heads)
    term[...] = dot(hid[...], grad_qkv[...], (0, 0)).astype(bf16)
    for j in range(chips):
        terms[j][...] = term[pl.ds(chip_of[j] * tall, tall), :]
    ghid[...] = dot(grad_qkv[...], weight[...], (1, 1))


def second_kernel(chips, rows, heads, fold, chip_of, seg_col, seg_row, hid, cots, proj, att_in, ghid, *refs):
    pieces, refs = refs[:chips], refs[chips:]
    own, peer, refs = *refs[:2], refs[2:]
    terms, refs = refs[:chips], refs[chips:]
    if fold:
        proj_out = None
    else:
        proj_out, refs = refs[0], refs[1:]
    weight, att, qkv, grads, grad_qkv, term, proj_term = refs
    width = heads * HEAD_DIM
    tall = pieces[0].shape[0]
    half = 3 * width
    for j in range(chips):
        weight[pl.ds(chip_of[j] * tall, tall), :] = pieces[j][...]
    qkv[...] = dot(hid[...], weight[...], (1, 0)).astype(bf16)
    grads[...] = dot(cots[...], proj[...], (1, 1)).astype(bf16)
    attention(qkv, grads, seg_col, seg_row, att, grad_qkv, rows, heads)
    proj_term[:width, :] = dot(att_in[...], cots[...], (0, 0)).astype(bf16)
    proj_term[width:, :] = dot(att[...], cots[...], (0, 0)).astype(bf16)
    term[...] = dot(hid[...], grad_qkv[...], (0, 0)).astype(bf16)
    for j in range(chips):
        at = chip_of[j]
        terms[j][:, :half] = term[pl.ds(at * tall, tall), :]
        if fold:
            low = tall // 2
            side = cots.shape[1] // 2
            terms[j][:low, half:] = proj_term[pl.ds(at * low, low), :side]
            terms[j][low:, half:] = proj_term[pl.ds(at * low, low), side:]
    if not fold:
        proj_out[...] = proj_term[...]
    own[...] = ghid[:rows, :] + dot(grad_qkv[:rows, :], weight[...], (1, 1))
    peer[...] = (ghid[rows:, :] + dot(grad_qkv[rows:, :], weight[...], (1, 1))).astype(bf16)


def last_kernel(tokens, cot, vec, own, peer, grad, terms):
    step = 64
    terms[...] = jnp.zeros_like(terms)

    def chunk(i, carry):
        at = pl.ds(i * step, step)
        source = tokens[at, :].astype(f32)
        centered = source - jnp.mean(source, axis=1, keepdims=True)
        variance = jnp.mean(centered * centered, axis=1, keepdims=True)
        inverse = lax.rsqrt(variance + norm_eps)
        normed = centered * inverse
        grad_hidden = own[at, :] + peer[at, :].astype(f32)
        terms[0:1, :] += jnp.sum(grad_hidden * normed, axis=0, keepdims=True)
        terms[1:2, :] += jnp.sum(grad_hidden, axis=0, keepdims=True)
        grad_normed = grad_hidden * vec[0:1, :]
        inner = grad_normed - jnp.mean(grad_normed, axis=1, keepdims=True)
        inner = inner - normed * jnp.mean(grad_normed * normed, axis=1, keepdims=True)
        grad[at, :] = (cot[at, :].astype(f32) + inverse * inner).astype(bf16)
        return carry

    lax.fori_loop(0, tokens.shape[0] // step, chunk, 0)


SMEM = pl.BlockSpec(memory_space=pltpu.SMEM)
VMEM = pl.BlockSpec(memory_space=pltpu.VMEM)


def call(body, name, scratch, outs, flops, *args):
    shapes = [jax.ShapeDtypeStruct(s, t) for s, t in outs]
    specs = [SMEM if a.ndim == 1 else VMEM for a in args]
    return pl.pallas_call(
        body,
        name=name,
        out_shape=shapes,
        in_specs=specs,
        out_specs=[VMEM] * len(shapes),
        scratch_shapes=[pltpu.VMEM(s, t) for s, t in scratch],
        cost_estimate=pl.CostEstimate(flops=flops, bytes_accessed=1 << 23, transcendentals=0),
        compiler_params=pltpu.CompilerParams(vmem_limit_bytes=56 << 20),
    )(*args)


def per_device(
    tokens, cotangent, patch_count, image_starts, qkv_weight, proj_weight, norm_gain, norm_shift
):
    rows, d = tokens.shape
    own_rows = qkv_weight.shape[0]
    owners, replicas = lax.axis_size("fsdp"), lax.axis_size("dp")
    chips = owners // 2
    me = lax.axis_index("fsdp")
    chip, even = me // 2, me % 2 == 0
    place = ring_place(chip, chips)
    heads = d // HEAD_DIM // 4
    width = heads * HEAD_DIM
    fold = own_rows == HEAD_DIM
    tall = 2 * own_rows

    parts = qkv_weight.reshape(own_rows, 3, 2, heads, 2, HEAD_DIM).transpose(4, 0, 2, 1, 3, 5)
    parts = parts.reshape(2, own_rows, 6 * width)
    mine, others = jnp.where(even, parts[0], parts[1]), jnp.where(even, parts[1], parts[0])
    got = swap_cores(others)
    block = jnp.where(
        even, jnp.concatenate([mine, got], axis=0), jnp.concatenate([got, mine], axis=0)
    )
    block_a, block_b = block[:, : 3 * width], block[:, 3 * width :]
    if fold:
        side = jnp.concatenate([proj_weight[:, : d // 2], proj_weight[:, d // 2 :]], axis=0)
        block_a = jnp.concatenate([block_a, side], axis=1)
    pieces_a = ring_gather(block_a, chips, True)
    pieces_b = ring_gather(block_b, chips, False)

    vec = jnp.zeros((2, owners, own_rows), bf16)
    vec = lax.dynamic_update_slice(vec, jnp.stack([norm_gain, norm_shift])[:, None], (0, me, 0))
    vec = small_sum(vec.reshape(2, d), ("fsdp",)).astype(f32)

    position = jnp.arange(rows, dtype=jnp.int32)
    live = position < patch_count[0]
    segment = jnp.sum((image_starts[0][None, :] <= position[:, None]).astype(jnp.int32), axis=1)
    segment = jnp.where(live, segment, image_starts.shape[1] + 1)
    masked_cot = jnp.where(live[:, None], cotangent, jnp.zeros_like(cotangent))
    segments = jnp.stack([segment, swap_cores(segment)])
    both = jnp.concatenate([tokens, swap_cores(tokens)], axis=0)
    cots = jnp.concatenate([masked_cot, swap_cores(masked_cot)], axis=0)
    seg_col, seg_row = segments.reshape(2 * rows, 1), segments.reshape(2, 1, rows)

    def table(wide):
        offs = jnp.array(offsets(chips, wide), jnp.int32)
        return ring_chip((place + offs) % chips, chips).astype(jnp.int32)

    table_a, table_b = table(True), table(False)
    work = 2 * rows * 2 * (d * 3 * width * 3 + d * width * 3 + 6 * heads * rows * 2 * HEAD_DIM)
    scratch = [
        ((2 * rows, 3 * width), bf16),
        ((2 * rows, width), bf16),
        ((2 * rows, 3 * width), bf16),
        ((d, 3 * width), bf16),
    ]
    extra = []
    if not fold:
        proj = lax.all_gather(proj_weight, "fsdp", axis=0, tiled=True)
        proj = proj.reshape(2 * heads, 2, HEAD_DIM, d)
        extra = [jnp.where(even, proj[:, 0], proj[:, 1]).reshape(2 * width, d)]
    hid, att, ghid, proj_rest, *terms_a = call(
        functools.partial(first_kernel, chips, rows, heads, fold),
        "first",
        [((d, 3 * width), bf16), ((2 * width, d), bf16)] + scratch,
        [((2 * rows, d), bf16), ((2 * rows, width), bf16), ((2 * rows, d), f32), ((width, d), bf16)]
        + [((tall, 3 * width), bf16)] * chips,
        work,
        *(table_a, seg_col, seg_row, both, cots, vec, *pieces_a, *extra),
    )
    wide_b = 3 * width + (d // 2 if fold else 0)
    own, peer, *terms_b = call(
        functools.partial(second_kernel, chips, rows, heads, fold),
        "second",
        [((d, 3 * width), bf16), ((2 * rows, width), bf16)] + scratch + [((2 * width, d), bf16)],
        [((rows, d), f32), ((rows, d), bf16)]
        + [((tall, wide_b), bf16)] * chips
        + ([] if fold else [((2 * width, d), bf16)]),
        work,
        *(table_b, seg_col, seg_row, hid, cots, proj_rest, att, ghid, *pieces_b),
    )
    grad_block, vec_term = call(
        last_kernel,
        "last",
        [],
        [((rows, d), bf16), ((2, d), f32)],
        1 << 24,
        *(tokens, cotangent, vec, own, swap_cores(peer)),
    )

    scale = 1.0 / math.sqrt(rows * replicas * owners)
    sum_a = replica_sum(ring_scatter(terms_a[:chips], chips, True))
    sum_b = replica_sum(ring_scatter(terms_b[:chips], chips, False))
    if fold:
        side = sum_b[:, 3 * width :]
        proj_grad = jnp.concatenate([side[:own_rows], side[own_rows:]], axis=1) * scale
        sum_b = sum_b[:, : 3 * width]
    else:
        proj_term = terms_b[chips].reshape(2 * heads, HEAD_DIM, d)
        none = jnp.zeros_like(proj_term)
        spread = jnp.stack(
            [jnp.where(even, proj_term, none), jnp.where(even, none, proj_term)], axis=1
        )
        o_sum = lax.psum_scatter(spread.reshape(d, d), "fsdp", scatter_dimension=0, tiled=True)
        proj_grad = replica_sum(o_sum) * scale
    q_sum = jnp.concatenate([sum_a, sum_b], axis=1) * scale
    low, high = q_sum[:own_rows], q_sum[own_rows:]
    keep, give = jnp.where(even, low, high), jnp.where(even, high, low)
    got = swap_cores(give)
    pair = jnp.stack([jnp.where(even, keep, got), jnp.where(even, got, keep)])
    pair = pair.reshape(2, own_rows, 2, 3, heads, HEAD_DIM).transpose(1, 3, 2, 4, 0, 5)
    qkv_grad = pair.reshape(own_rows, 12 * width)
    vec_sum = small_sum(vec_term, ("fsdp", "dp")) * scale
    vec_own = lax.dynamic_slice(vec_sum, (0, me * own_rows), (2, own_rows))
    return grad_block, qkv_grad, proj_grad, vec_own[0], vec_own[1]


def solution(mesh):
    both = P(("dp", "fsdp"))
    rows2 = P(("dp", "fsdp"), None)
    own2, own = P("fsdp", None), P("fsdp")
    return jax.shard_map(
        per_device,
        mesh=mesh,
        in_specs=(rows2, rows2, both, rows2, own2, own2, own, own),
        out_specs=(rows2, own2, own2, own, own),
        check_vma=False,
    )
```

```python
import functools
import math

import jax
import jax.numpy as jnp
from jax import lax
from jax.experimental import pallas as pl
from jax.experimental.pallas import tpu as pltpu
from jax.sharding import PartitionSpec as P

HEAD_DIM = 64
norm_eps = 1e-06
masked_score = -1e30
bf16 = jnp.bfloat16
f32 = jnp.float32
SPARE = 12 << 20


def ring_chips(chips):
    if chips % 2:
        return list(range(chips))
    half = chips // 2
    return [2 * i for i in range(half)] + [2 * i + 1 for i in reversed(range(half))]


def ring_place(chip, chips):
    if chips % 2:
        return chip
    return jnp.where(chip % 2 == 0, chip // 2, chips - 1 - chip // 2)


def ring_chip(place, chips):
    if chips % 2:
        return place
    return jnp.where(place < chips // 2, 2 * place, 2 * (chips - 1 - place) + 1)


def ring_step(x, chips, step):
    order = ring_chips(chips)
    pairs = [
        (2 * order[i] + c, 2 * order[(i + step) % chips] + c) for i in range(chips) for c in range(2)
    ]
    return lax.ppermute(x, "fsdp", pairs)


def swap_bit(x, axis, bit):
    n = lax.axis_size(axis)
    return lax.ppermute(x, axis, [(i, i ^ bit) for i in range(n)])


def swap_cores(x):
    return swap_bit(x, "fsdp", 1)


def swap_replica_and_core(x):
    n = lax.axis_size("fsdp")
    pairs = [(r * n + i, (1 - r) * n + (i ^ 1)) for r in range(2) for i in range(n)]
    return lax.ppermute(x, ("dp", "fsdp"), pairs)


def after(x, *first):
    return lax.optimization_barrier((x,) + first)[0]


def small_sum(x, axes):
    for axis in axes:
        n = lax.axis_size(axis)
        if n & (n - 1):
            x = lax.psum(x, axis)
            continue
        bit = 1
        while bit < n:
            x = x + swap_bit(x, axis, bit)
            bit *= 2
    return x


def reach(chips, step, wide):
    far, near = chips // 2, chips - 1 - chips // 2
    return far if (step < 0) == wide else near


def offsets(chips, wide):
    ahead, behind = reach(chips, -1, wide), reach(chips, 1, wide)
    return [0] + [-(s + 1) for s in range(ahead)] + [s + 1 for s in range(behind)]


def gather_step(state, chips, wide, *first):
    for step in (1, -1):
        got = state[step]
        if len(got) <= reach(chips, -step, wide):
            state[step] = got + [ring_step(after(got[-1], *first), chips, step)]


def gather_pieces(state):
    return [state[1][0]] + state[1][1:] + state[-1][1:]


class Scatter:
    def __init__(self, pieces, chips, wide):
        self.at = {o: pieces[i] for i, o in enumerate(offsets(chips, wide))}
        self.chips = chips
        self.left = {step: reach(chips, step, wide) for step in (1, -1)}
        self.held = {step: self.at[step * self.left[step]] for step in (1, -1)}

    def step(self, *first):
        for step in (1, -1):
            if not self.left[step]:
                continue
            got = ring_step(after(self.held[step], *first), self.chips, step)
            self.left[step] -= 1
            if self.left[step]:
                own = self.at[step * self.left[step]]
                got = (got.astype(f32) + own.astype(f32)).astype(bf16)
            self.held[step] = got

    def done(self):
        while self.left[1] or self.left[-1]:
            self.step()
        total = self.at[0].astype(f32) + self.held[1].astype(f32) + self.held[-1].astype(f32)
        return total.astype(bf16)


def dot(a, b, contract):
    return lax.dot_general(
        a, b, (((contract[0],), (contract[1],)), ((), ())), preferred_element_type=f32
    )


def segment_of(meta, part, position, starts):
    base = part * (starts + 1)
    segment = jnp.zeros_like(position)
    for j in range(starts):
        segment += (meta[base + 1 + j] <= position).astype(jnp.int32)
    return jnp.where(position < meta[base], segment, starts + 1)


def norm_kernel(starts, meta, tokens, peer, cot, peer_cot, vec, hid, cots):
    rows = tokens.shape[0]
    step = 64
    gain, shift = vec[0:1, :].astype(f32), vec[1:2, :].astype(f32)
    for part, (text, grad) in enumerate(((tokens, cot), (peer, peer_cot))):

        def norm(i, carry):
            at = pl.ds(i * step, step)
            to = pl.ds(part * rows + i * step, step)
            source = text[at, :].astype(f32)
            centered = source - jnp.mean(source, axis=1, keepdims=True)
            variance = jnp.mean(centered * centered, axis=1, keepdims=True)
            normed = centered * lax.rsqrt(variance + norm_eps)
            hid[to, :] = (normed * gain + shift).astype(bf16)
            position = i * step + lax.broadcasted_iota(jnp.int32, (step, grad.shape[1]), 0)
            kept = grad[at, :]
            cots[to, :] = jnp.where(
                position < meta[part * (starts + 1)], kept, jnp.zeros_like(kept)
            )
            return carry

        lax.fori_loop(0, rows // step, norm, 0)


def attend_kernel(rows, starts, heads, meta, qkv, grads, att, grad_qkv):
    width = heads * HEAD_DIM
    factor = HEAD_DIM ** (-0.5)
    lane = lax.broadcasted_iota(jnp.int32, (rows, 2 * HEAD_DIM), 1)

    def block(b, carry):
        at = pl.ds(b * rows, rows)
        seg_col = segment_of(meta, b, lax.broadcasted_iota(jnp.int32, (rows, 1), 0), starts)
        seg_row = segment_of(meta, b, lax.broadcasted_iota(jnp.int32, (1, rows), 1), starts)
        allowed = seg_col == seg_row
        for pair in range(heads // 2):
            lanes = pl.ds(pair * 2 * HEAD_DIM, 2 * HEAD_DIM)
            q = qkv[at, lanes]
            k = qkv[at, pl.ds(width + pair * 2 * HEAD_DIM, 2 * HEAD_DIM)]
            v = qkv[at, pl.ds(2 * width + pair * 2 * HEAD_DIM, 2 * HEAD_DIM)]
            g = grads[at, lanes]
            sums = None
            for side in range(2):
                pick = (lane < HEAD_DIM) if side == 0 else (lane >= HEAD_DIM)
                only = lambda x: jnp.where(pick, x, jnp.zeros_like(x))
                qs, ks, vs, gs = only(q), only(k), only(v), only(g)
                scores = dot(qs, k, (1, 1)) * factor
                scores = jnp.where(allowed, scores, masked_score)
                expon = jnp.exp(scores - jnp.max(scores, axis=1, keepdims=True))
                probs = expon * (1.0 / jnp.sum(expon, axis=1, keepdims=True))
                low = probs.astype(bf16)
                grad_probs = dot(gs, v, (1, 1))
                moved = jnp.sum(probs * grad_probs, axis=1, keepdims=True)
                grad_scores = (probs * (grad_probs - moved) * factor).astype(bf16)
                new = (
                    dot(low, vs, (1, 0)),
                    dot(grad_scores, ks, (1, 0)),
                    dot(grad_scores, qs, (0, 0)),
                    dot(low, gs, (0, 0)),
                )
                sums = new if sums is None else tuple(x + y for x, y in zip(sums, new))
            att[at, lanes] = sums[0].astype(bf16)
            for i in range(3):
                to = pl.ds(i * width + pair * 2 * HEAD_DIM, 2 * HEAD_DIM)
                grad_qkv[at, to] = sums[i + 1].astype(bf16)
        return carry

    lax.fori_loop(0, 2, block, 0)


def project_kernel(chips, half, fold, first, chip_of, hid, cots, *refs):
    proj_in = None
    if fold and first:
        proj = refs[-1]
    else:
        proj_in, refs = refs[0], refs[1:]
    pieces, refs = refs[:chips], refs[chips:]
    weight, qkv, grads = refs[:3]
    width = half // 3
    tall = pieces[0].shape[0]
    for j in range(chips):
        weight[pl.ds(chip_of[j] * tall, tall), :] = pieces[j][:, :half]
        if fold and first:
            low = tall // 2
            at = pl.ds(chip_of[j] * low, low)
            side = hid.shape[1] // 2
            proj[at, :side] = pieces[j][:low, half:]
            proj[at, side:] = pieces[j][low:, half:]
    source = proj if proj_in is None else proj_in
    mine = source[:width, :] if first else source[width:, :]
    qkv[...] = dot(hid[...], weight[...], (1, 0)).astype(bf16)
    grads[...] = dot(cots[...], mine, (1, 1)).astype(bf16)


def terms_kernel(chips, half, fold, last, chip_of, hid, grad_qkv, *refs):
    if last:
        (cots, att_a, att_b), refs = refs[:3], refs[3:]
    pieces, refs = refs[:chips], refs[chips:]
    term = refs[-1]
    tall = pieces[0].shape[0]
    if last:
        width = half // 3
        proj_term = refs[0] if not fold else refs[-2]
        proj_term[:width, :] = dot(att_a[...], cots[...], (0, 0)).astype(bf16)
        proj_term[width:, :] = dot(att_b[...], cots[...], (0, 0)).astype(bf16)
    term[...] = dot(hid[...], grad_qkv[...], (0, 0)).astype(bf16)
    for j in range(chips):
        at = chip_of[j]
        pieces[j][:, :half] = term[pl.ds(at * tall, tall), :]
        if last and fold:
            low = tall // 2
            side = cots.shape[1] // 2
            pieces[j][:low, half:] = proj_term[pl.ds(at * low, low), :side]
            pieces[j][low:, half:] = proj_term[pl.ds(at * low, low), side:]


def hidden_kernel(grad_a, weight_a, grad_b, weight_b, own, peer):
    rows = own.shape[0]
    both = lambda at: dot(grad_a[at, :], weight_a[...], (1, 1)) + dot(
        grad_b[at, :], weight_b[...], (1, 1)
    )
    peer[...] = both(pl.ds(rows, rows)).astype(bf16)
    own[...] = both(pl.ds(0, rows))


def last_kernel(tokens, cot, vec, own, peer, grad, terms):
    step = 64
    terms[...] = jnp.zeros_like(terms)
    gain = vec[0:1, :].astype(f32)

    def chunk(i, carry):
        at = pl.ds(i * step, step)
        source = tokens[at, :].astype(f32)
        centered = source - jnp.mean(source, axis=1, keepdims=True)
        variance = jnp.mean(centered * centered, axis=1, keepdims=True)
        inverse = lax.rsqrt(variance + norm_eps)
        normed = centered * inverse
        grad_hidden = own[at, :] + peer[at, :].astype(f32)
        terms[0:1, :] += jnp.sum(grad_hidden * normed, axis=0, keepdims=True)
        terms[1:2, :] += jnp.sum(grad_hidden, axis=0, keepdims=True)
        grad_normed = grad_hidden * gain
        inner = grad_normed - jnp.mean(grad_normed, axis=1, keepdims=True)
        inner = inner - normed * jnp.mean(grad_normed * normed, axis=1, keepdims=True)
        grad[at, :] = (cot[at, :].astype(f32) + inverse * inner).astype(bf16)
        return carry

    lax.fori_loop(0, tokens.shape[0] // step, chunk, 0)


def finish_kernel(heads, scale, parity, own_a, alt_a, own_b, alt_b, grad):
    rows = grad.shape[0]
    width = heads * HEAD_DIM
    swapped = jnp.full((rows, 2 * HEAD_DIM), parity[0], jnp.int32) == 1
    low = lax.broadcasted_iota(jnp.int32, (rows, 2 * HEAD_DIM), 1) < HEAD_DIM
    for g, (own, alt) in enumerate(((own_a, alt_a), (own_b, alt_b))):
        for i in range(3):
            for pair in range(heads // 2):
                lanes = pl.ds(i * width + pair * 2 * HEAD_DIM, 2 * HEAD_DIM)
                x, y = own[:, lanes] * scale, alt[:, lanes] * scale
                ev, od = jnp.where(swapped, y, x), jnp.where(swapped, x, y)
                base = i * 4 * width + g * 2 * width + pair * 4 * HEAD_DIM
                roll = lambda z: pltpu.roll(z, HEAD_DIM, 1)
                grad[:, pl.ds(base, 2 * HEAD_DIM)] = jnp.where(low, ev, roll(od))
                grad[:, pl.ds(base + 2 * HEAD_DIM, 2 * HEAD_DIM)] = jnp.where(low, roll(ev), od)


SMEM = pl.BlockSpec(memory_space=pltpu.SMEM)
VMEM = pl.BlockSpec(memory_space=pltpu.VMEM)


def size_of(shape, kind):
    return math.prod(shape) * jnp.dtype(kind).itemsize


def call(body, name, scratch, outs, flops, *args):
    shapes = [jax.ShapeDtypeStruct(s, t) for s, t in outs]
    specs = [SMEM if a.ndim == 1 else VMEM for a in args]
    need = sum(size_of(s, t) for s, t in outs + scratch) + sum(size_of(a.shape, a.dtype) for a in args)
    return pl.pallas_call(
        body,
        name=name,
        out_shape=shapes,
        in_specs=specs,
        out_specs=[VMEM] * len(shapes),
        scratch_shapes=[pltpu.VMEM(s, t) for s, t in scratch],
        cost_estimate=pl.CostEstimate(flops=flops, bytes_accessed=need, transcendentals=0),
        compiler_params=pltpu.CompilerParams(vmem_limit_bytes=need + SPARE),
    )(*args)


def per_device(
    tokens, cotangent, patch_count, image_starts, qkv_weight, proj_weight, norm_gain, norm_shift
):
    rows, d = tokens.shape
    own_rows = qkv_weight.shape[0]
    owners, replicas = lax.axis_size("fsdp"), lax.axis_size("dp")
    chips = owners // 2
    me = lax.axis_index("fsdp")
    chip, even = me // 2, me % 2 == 0
    place = ring_place(chip, chips)
    heads = d // HEAD_DIM // 4
    width = heads * HEAD_DIM
    half = 3 * width
    fold = own_rows == HEAD_DIM
    tall = 2 * own_rows
    starts = image_starts.shape[1]

    parts = qkv_weight.reshape(own_rows, 3, 2, heads, 2, HEAD_DIM).transpose(4, 0, 2, 1, 3, 5)
    parts = parts.reshape(2, own_rows, 2 * half)
    mine, others = jnp.where(even, parts[0], parts[1]), jnp.where(even, parts[1], parts[0])
    got = swap_cores(others)
    block = jnp.where(
        even, jnp.concatenate([mine, got], axis=0), jnp.concatenate([got, mine], axis=0)
    )
    block_a, block_b = block[:, :half], block[:, half:]
    if fold:
        side = jnp.concatenate([proj_weight[:, : d // 2], proj_weight[:, d // 2 :]], axis=0)
        block_a = jnp.concatenate([block_a, side], axis=1)
    gather_a = {1: [block_a], -1: [block_a]}
    gather_b = {1: [block_b], -1: [block_b]}
    far = chips // 2
    for _ in range(far):
        gather_step(gather_a, chips, True)
    pieces_a = gather_pieces(gather_a)
    if far > 1:
        gather_step(gather_b, chips, False, gather_a[1][-2])
    gather_step(gather_b, chips, False)

    vec = jnp.zeros((2, owners, own_rows), bf16)
    vec = lax.dynamic_update_slice(vec, jnp.stack([norm_gain, norm_shift])[:, None], (0, me, 0))
    vec = small_sum(vec.reshape(2, d), ("fsdp",))
    meta = jnp.concatenate([patch_count, image_starts[0]])
    meta = jnp.concatenate([meta, swap_cores(meta)])

    def table(wide):
        offs = jnp.array(offsets(chips, wide), jnp.int32)
        return ring_chip((place + offs) % chips, chips).astype(jnp.int32)

    table_a, table_b = table(True), table(False)
    two = 2 * rows
    wide_a = two * d * 2
    hid, cots = call(
        functools.partial(norm_kernel, starts), "norm", [],
        [((two, d), bf16)] * 2, two * d * 20,
        meta, tokens, swap_cores(tokens), cotangent, swap_cores(cotangent), vec,
    )
    extra = []
    if not fold:
        proj = lax.all_gather(proj_weight, "fsdp", axis=0, tiled=True)
        proj = proj.reshape(2 * heads, 2, HEAD_DIM, d)
        extra = [jnp.where(even, proj[:, 0], proj[:, 1]).reshape(2 * width, d)]
    projected = [((d, half), bf16), ((two, half), bf16), ((two, width), bf16)]

    def project(first, chip_of, proj, pieces):
        return call(
            functools.partial(project_kernel, chips, half, fold, first), "project", [],
            projected + ([((2 * width, d), bf16)] if fold and first else []),
            wide_a * (half + width), chip_of, hid, cots, *proj, *pieces,
        )

    def attend(qkv, grads):
        return call(
            functools.partial(attend_kernel, rows, starts, heads), "attend", [],
            [((two, width), bf16), ((two, half), bf16)], two * rows * heads * HEAD_DIM * 48,
            meta, qkv, grads,
        )

    def terms(last, chip_of, grad_qkv, *more):
        broad = half + (d // 2 if last and fold else 0)
        proj_shape = [((2 * width, d), bf16)] if last else []
        return call(
            functools.partial(terms_kernel, chips, half, fold, last), "terms",
            (proj_shape if fold else []) + [((d, half), bf16)],
            [((tall, broad), bf16)] * chips + ([] if fold else proj_shape),
            wide_a * half, chip_of, hid, grad_qkv, *more,
        )

    weight_a, qkv_a, grads_a, *proj = project(True, table_a, extra, pieces_a)
    proj = proj if fold else extra
    gather_step(gather_b, chips, False, grads_a)
    att_a, grad_a = attend(qkv_a, grads_a)
    for _ in range(far):
        gather_step(gather_b, chips, False, att_a)
    pieces_b = gather_pieces(gather_b)
    scatter_a = Scatter(terms(False, table_a, grad_a), chips, True)
    scatter_a.step()
    weight_b, qkv_b, grads_b = project(False, table_b, proj, pieces_b)
    scatter_a.step(grads_b)
    att_b, grad_b = attend(qkv_b, grads_b)
    scatter_a.step(att_b)
    terms_b = terms(True, table_b, grad_b, cots, att_a, att_b)
    scatter_b = Scatter(terms_b[:chips], chips, False)
    scatter_b.step()
    sum_a = scatter_a.done()
    own, peer = call(
        hidden_kernel, "hidden", [], [((rows, d), f32), ((rows, d), bf16)],
        wide_a * half * 2, after(grad_a, terms_b[0]), weight_a, grad_b, weight_b,
    )
    grad_block, vec_term = call(
        last_kernel, "last", [], [((rows, d), bf16), ((2, d), f32)], rows * d * 40,
        tokens, cotangent, vec, own, swap_cores(peer),
    )
    sum_b = scatter_b.done()

    scale = 1.0 / math.sqrt(rows * replicas * owners)

    def settle(total):
        low, high = total[:own_rows, :half], total[own_rows:, :half]
        keep, give = jnp.where(even, low, high), jnp.where(even, high, low)
        if replicas == 2:
            mine = keep.astype(f32) + swap_bit(keep, "dp", 1).astype(f32)
            alt = swap_cores(give).astype(f32) + swap_replica_and_core(give).astype(f32)
            return mine, alt
        mine, give = lax.psum(keep, "dp"), lax.psum(give, "dp")
        return mine.astype(f32), swap_cores(give).astype(f32)

    if fold:
        side = sum_b[:, half:]
        o_sum = jnp.concatenate([side[:own_rows], side[own_rows:]], axis=1)
    else:
        proj_term = terms_b[chips].reshape(2 * heads, HEAD_DIM, d)
        none = jnp.zeros_like(proj_term)
        spread = jnp.stack(
            [jnp.where(even, proj_term, none), jnp.where(even, none, proj_term)], axis=1
        )
        o_sum = lax.psum_scatter(spread.reshape(d, d), "fsdp", scatter_dimension=0, tiled=True)
    if replicas == 2:
        proj_grad = (o_sum.astype(f32) + swap_bit(o_sum, "dp", 1).astype(f32)) * scale
    else:
        proj_grad = lax.psum(o_sum, "dp").astype(f32) * scale
    parity = (me % 2).astype(jnp.int32).reshape(1)
    (qkv_grad,) = call(
        functools.partial(finish_kernel, heads, scale), "finish", [],
        [((own_rows, 4 * half), f32)], own_rows * half * 40,
        parity, *settle(sum_a), *settle(sum_b),
    )
    vec_sum = small_sum(vec_term, ("fsdp", "dp")) * scale
    vec_own = lax.dynamic_slice(vec_sum, (0, me * own_rows), (2, own_rows))
    return grad_block, qkv_grad, proj_grad, vec_own[0], vec_own[1]


def solution(mesh):
    both = P(("dp", "fsdp"))
    rows2 = P(("dp", "fsdp"), None)
    own2, own = P("fsdp", None), P("fsdp")
    return jax.shard_map(
        per_device,
        mesh=mesh,
        in_specs=(rows2, rows2, both, rows2, own2, own2, own, own),
        out_specs=(rows2, own2, own2, own, own),
        check_vma=False,
    )
```

```python
import functools
import math

import jax
import jax.numpy as jnp
from jax import lax
from jax.experimental import pallas as pl
from jax.experimental.pallas import tpu as pltpu
from jax.sharding import PartitionSpec as P

HEAD_DIM = 64
norm_eps = 1e-06
masked_score = -1e30
bf16 = jnp.bfloat16
f32 = jnp.float32
SPARE = 12 << 20


def ring_chips(chips):
    if chips % 2:
        return list(range(chips))
    half = chips // 2
    return [2 * i for i in range(half)] + [2 * i + 1 for i in reversed(range(half))]


def ring_place(chip, chips):
    if chips % 2:
        return chip
    return jnp.where(chip % 2 == 0, chip // 2, chips - 1 - chip // 2)


def ring_chip(place, chips):
    if chips % 2:
        return place
    return jnp.where(place < chips // 2, 2 * place, 2 * (chips - 1 - place) + 1)


def ring_step(x, chips, step):
    order = ring_chips(chips)
    pairs = [
        (2 * order[i] + c, 2 * order[(i + step) % chips] + c) for i in range(chips) for c in range(2)
    ]
    return lax.ppermute(x, "fsdp", pairs)


def swap_bit(x, axis, bit):
    n = lax.axis_size(axis)
    return lax.ppermute(x, axis, [(i, i ^ bit) for i in range(n)])


def swap_cores(x):
    return swap_bit(x, "fsdp", 1)


def swap_replica_and_core(x):
    n = lax.axis_size("fsdp")
    pairs = [(r * n + i, (1 - r) * n + (i ^ 1)) for r in range(2) for i in range(n)]
    return lax.ppermute(x, ("dp", "fsdp"), pairs)


def after(x, *first):
    return lax.optimization_barrier((x,) + first)[0]


def small_sum(x, axes):
    for axis in axes:
        n = lax.axis_size(axis)
        if n & (n - 1):
            x = lax.psum(x, axis)
            continue
        bit = 1
        while bit < n:
            x = x + swap_bit(x, axis, bit)
            bit *= 2
    return x


def reach(chips, step, wide):
    far, near = chips // 2, chips - 1 - chips // 2
    return far if (step < 0) == wide else near


def offsets(chips, wide):
    ahead, behind = reach(chips, -1, wide), reach(chips, 1, wide)
    return [0] + [-(s + 1) for s in range(ahead)] + [s + 1 for s in range(behind)]


def gather_step(state, chips, wide, *first):
    for step in (1, -1):
        got = state[step]
        if len(got) <= reach(chips, -step, wide):
            state[step] = got + [ring_step(after(got[-1], *first), chips, step)]


def gather_pieces(state):
    return [state[1][0]] + state[1][1:] + state[-1][1:]


def total_of(*terms):
    total = terms[0].astype(f32)
    for term in terms[1:]:
        total = total + term.astype(f32)
    return total.astype(bf16)


class Scatter:
    def __init__(self, at, chips, wide):
        self.at, self.chips = at, chips
        self.left = {step: reach(chips, step, wide) for step in (1, -1)}
        self.held = {}
        for step in (1, -1):
            terms = at[step * self.left[step]]
            self.held[step] = terms[0] if len(terms) == 1 else total_of(*terms)

    def step(self):
        for step in (1, -1):
            if not self.left[step]:
                continue
            got = ring_step(self.held[step], self.chips, step)
            self.left[step] -= 1
            if self.left[step]:
                got = total_of(got, *self.at[step * self.left[step]])
            self.held[step] = got

    def done(self):
        while self.left[1] or self.left[-1]:
            self.step()
        return total_of(*self.at[0], self.held[1], self.held[-1])


def dot(a, b, contract):
    return lax.dot_general(
        a, b, (((contract[0],), (contract[1],)), ((), ())), preferred_element_type=f32
    )


def segment_of(meta, part, position, starts):
    base = part * (starts + 1)
    segment = jnp.zeros_like(position)
    for j in range(starts):
        segment += (meta[base + 1 + j] <= position).astype(jnp.int32)
    return jnp.where(position < meta[base], segment, starts + 1)


def norm_kernel(starts, meta, tokens, peer, cot, peer_cot, normed, cots):
    rows = tokens.shape[0]
    step = 64
    for part, (text, grad) in enumerate(((tokens, cot), (peer, peer_cot))):

        def norm(i, carry):
            at = pl.ds(i * step, step)
            to = pl.ds(part * rows + i * step, step)
            source = text[at, :].astype(f32)
            centered = source - jnp.mean(source, axis=1, keepdims=True)
            variance = jnp.mean(centered * centered, axis=1, keepdims=True)
            normed[to, :] = centered * lax.rsqrt(variance + norm_eps)
            position = i * step + lax.broadcasted_iota(jnp.int32, (step, grad.shape[1]), 0)
            kept = grad[at, :]
            cots[to, :] = jnp.where(
                position < meta[part * (starts + 1)], kept, jnp.zeros_like(kept)
            )
            return carry

        lax.fori_loop(0, rows // step, norm, 0)


def attend_kernel(rows, starts, heads, meta, qkv, grads, att, grad_qkv):
    width = heads * HEAD_DIM
    factor = HEAD_DIM ** (-0.5)
    lane = lax.broadcasted_iota(jnp.int32, (rows, 2 * HEAD_DIM), 1)

    def block(b, carry):
        at = pl.ds(b * rows, rows)
        seg_col = segment_of(meta, b, lax.broadcasted_iota(jnp.int32, (rows, 1), 0), starts)
        seg_row = segment_of(meta, b, lax.broadcasted_iota(jnp.int32, (1, rows), 1), starts)
        allowed = seg_col == seg_row
        for pair in range(heads // 2):
            lanes = pl.ds(pair * 2 * HEAD_DIM, 2 * HEAD_DIM)
            q = qkv[at, lanes]
            k = qkv[at, pl.ds(width + pair * 2 * HEAD_DIM, 2 * HEAD_DIM)]
            v = qkv[at, pl.ds(2 * width + pair * 2 * HEAD_DIM, 2 * HEAD_DIM)]
            g = grads[at, lanes]
            sums = None
            for side in range(2):
                pick = (lane < HEAD_DIM) if side == 0 else (lane >= HEAD_DIM)
                only = lambda x: jnp.where(pick, x, jnp.zeros_like(x))
                qs, ks, vs, gs = only(q), only(k), only(v), only(g)
                scores = dot(qs, k, (1, 1)) * factor
                scores = jnp.where(allowed, scores, masked_score)
                expon = jnp.exp(scores - jnp.max(scores, axis=1, keepdims=True))
                probs = expon * (1.0 / jnp.sum(expon, axis=1, keepdims=True))
                low = probs.astype(bf16)
                grad_probs = dot(gs, v, (1, 1))
                moved = jnp.sum(probs * grad_probs, axis=1, keepdims=True)
                grad_scores = (probs * (grad_probs - moved) * factor).astype(bf16)
                new = (
                    dot(low, vs, (1, 0)),
                    dot(grad_scores, ks, (1, 0)),
                    dot(grad_scores, qs, (0, 0)),
                    dot(low, gs, (0, 0)),
                )
                sums = new if sums is None else tuple(x + y for x, y in zip(sums, new))
            att[at, lanes] = sums[0].astype(bf16)
            for i in range(3):
                to = pl.ds(i * width + pair * 2 * HEAD_DIM, 2 * HEAD_DIM)
                grad_qkv[at, to] = sums[i + 1].astype(bf16)
        return carry

    lax.fori_loop(0, 2, block, 0)


def project_first_kernel(plan, at_q, at_p, side, normed, cots, *refs):
    chips, half, tall, fold, packed = plan
    pieces, refs = refs[:chips], refs[chips:]
    if fold:
        slabs, refs = refs[:chips], refs[chips:]
    else:
        proj_in, refs = refs[0], refs[1:]
    if not packed:
        vec_in, refs = refs[0], refs[1:]
    weight, qkv, grads, hid, proj, vec = refs
    width = half // 3
    for j in range(chips):
        weight[pl.ds(at_q[j] * tall, tall), :] = pieces[j][:tall, :]
        if packed:
            lanes = pl.ds(pl.multiple_of(at_q[j] * tall, tall), tall)
            vec[0:1, lanes] = pieces[j][tall : tall + 1, :tall].astype(f32)
            vec[1:2, lanes] = pieces[j][tall : tall + 1, tall : 2 * tall].astype(f32)
        if fold:
            proj[pl.ds(at_p[j] * HEAD_DIM, HEAD_DIM), :] = slabs[j][...]
    if not fold:
        proj[...] = proj_in[...]
    if not packed:
        vec[...] = vec_in[...].astype(f32)
    step = 64

    def scale(i, carry):
        at = pl.ds(i * step, step)
        hid[at, :] = (normed[at, :] * vec[0:1, :] + vec[1:2, :]).astype(bf16)
        return carry

    lax.fori_loop(0, normed.shape[0] // step, scale, 0)
    qkv[...] = dot(hid[...], weight[...], (1, 0)).astype(bf16)
    grads[...] = dot(cots[...], proj[pl.ds(side[0] * width, width), :], (1, 1)).astype(bf16)


def project_second_kernel(plan, at_q, side, hid, cots, proj, *refs):
    chips, half, tall, _, _ = plan
    pieces, (weight, qkv, grads) = refs[:chips], refs[chips:]
    width = half // 3
    for j in range(chips):
        weight[pl.ds(at_q[j] * tall, tall), :] = pieces[j][:tall, :]
    qkv[...] = dot(hid[...], weight[...], (1, 0)).astype(bf16)
    other = 1 - side[0]
    grads[...] = dot(cots[...], proj[pl.ds(other * width, width), :], (1, 1)).astype(bf16)


def terms_first_kernel(plan, order, at_q, hid, grad_qkv, *refs):
    tall = plan[2]
    outs, term = refs[:-1], refs[-1]
    term[...] = dot(hid[...], grad_qkv[...], (0, 0)).astype(bf16)
    for out, js in zip(outs, order):
        for i, j in enumerate(js):
            out[pl.ds(i * tall, tall), :] = term[pl.ds(at_q[j] * tall, tall), :]


def terms_second_kernel(plan, at_q, at_p, side, hid, grad_qkv, cots, att_first, att_second, *refs):
    chips, half, tall, fold, _ = plan
    width = half // 3
    pieces, refs = refs[:chips], refs[chips:]
    if fold:
        slabs, refs = refs[:chips], refs[chips:]
        term, proj_term = refs
    else:
        proj_term, term = refs
    term[...] = dot(hid[...], grad_qkv[...], (0, 0)).astype(bf16)
    at = side[0] * width
    proj_term[pl.ds(at, width), :] = dot(att_first[...], cots[...], (0, 0)).astype(bf16)
    proj_term[pl.ds(width - at, width), :] = dot(att_second[...], cots[...], (0, 0)).astype(bf16)
    for j in range(chips):
        pieces[j][...] = term[pl.ds(at_q[j] * tall, tall), :]
        if fold:
            slabs[j][...] = proj_term[pl.ds(at_p[j] * HEAD_DIM, HEAD_DIM), :]


def hidden_kernel(grad_a, weight_a, grad_b, weight_b, own, peer):
    rows = own.shape[0]
    both = lambda at: dot(grad_a[at, :], weight_a[...], (1, 1)) + dot(
        grad_b[at, :], weight_b[...], (1, 1)
    )
    peer[...] = both(pl.ds(rows, rows)).astype(bf16)
    own[...] = both(pl.ds(0, rows))


def last_kernel(tokens, cot, vec, own, peer, grad, terms):
    step = 64
    terms[...] = jnp.zeros_like(terms)
    gain = vec[0:1, :]

    def chunk(i, carry):
        at = pl.ds(i * step, step)
        source = tokens[at, :].astype(f32)
        centered = source - jnp.mean(source, axis=1, keepdims=True)
        variance = jnp.mean(centered * centered, axis=1, keepdims=True)
        inverse = lax.rsqrt(variance + norm_eps)
        normed = centered * inverse
        grad_hidden = own[at, :] + peer[at, :].astype(f32)
        terms[0:1, :] += jnp.sum(grad_hidden * normed, axis=0, keepdims=True)
        terms[1:2, :] += jnp.sum(grad_hidden, axis=0, keepdims=True)
        grad_normed = grad_hidden * gain
        inner = grad_normed - jnp.mean(grad_normed, axis=1, keepdims=True)
        inner = inner - normed * jnp.mean(grad_normed * normed, axis=1, keepdims=True)
        grad[at, :] = (cot[at, :].astype(f32) + inverse * inner).astype(bf16)
        return carry

    lax.fori_loop(0, tokens.shape[0] // step, chunk, 0)


def finish_kernel(heads, scale, flags, own_first, alt_first, own_second, alt_second, grad):
    rows = grad.shape[0]
    width = heads * HEAD_DIM
    flag = lambda i: jnp.full((rows, 2 * HEAD_DIM), flags[i], jnp.int32) == 1
    odd, turned = flag(0), flag(1)
    low = lax.broadcasted_iota(jnp.int32, (rows, 2 * HEAD_DIM), 1) < HEAD_DIM
    roll = lambda z: pltpu.roll(z, HEAD_DIM, 1)
    for i in range(3):
        for pair in range(heads // 2):
            lanes = pl.ds(i * width + pair * 2 * HEAD_DIM, 2 * HEAD_DIM)
            own = own_first[:, lanes].astype(f32) * scale, own_second[:, lanes].astype(f32) * scale
            alt = alt_first[:, lanes].astype(f32) * scale, alt_second[:, lanes].astype(f32) * scale
            for g in range(2):
                x = jnp.where(turned, own[1 - g], own[g])
                y = jnp.where(turned, alt[1 - g], alt[g])
                ev, od = jnp.where(odd, y, x), jnp.where(odd, x, y)
                base = i * 4 * width + g * 2 * width + pair * 4 * HEAD_DIM
                grad[:, pl.ds(base, 2 * HEAD_DIM)] = jnp.where(low, ev, roll(od))
                grad[:, pl.ds(base + 2 * HEAD_DIM, 2 * HEAD_DIM)] = jnp.where(low, roll(ev), od)


SMEM = pl.BlockSpec(memory_space=pltpu.SMEM)
VMEM = pl.BlockSpec(memory_space=pltpu.VMEM)


def size_of(shape, kind):
    return math.prod(shape) * jnp.dtype(kind).itemsize


def call(body, name, scratch, outs, flops, *args):
    shapes = [jax.ShapeDtypeStruct(s, t) for s, t in outs]
    specs = [SMEM if a.ndim == 1 else VMEM for a in args]
    need = sum(size_of(s, t) for s, t in outs + scratch) + sum(size_of(a.shape, a.dtype) for a in args)
    return pl.pallas_call(
        body,
        name=name,
        out_shape=shapes,
        in_specs=specs,
        out_specs=[VMEM] * len(shapes),
        scratch_shapes=[pltpu.VMEM(s, t) for s, t in scratch],
        cost_estimate=pl.CostEstimate(flops=flops, bytes_accessed=need, transcendentals=0),
        compiler_params=pltpu.CompilerParams(vmem_limit_bytes=need + SPARE),
    )(*args)


def per_device(
    tokens, cotangent, patch_count, image_starts, qkv_weight, proj_weight, norm_gain, norm_shift
):
    rows, d = tokens.shape
    own_rows = qkv_weight.shape[0]
    owners, replicas = lax.axis_size("fsdp"), lax.axis_size("dp")
    paired = replicas == 2
    chips = owners // 2
    me = lax.axis_index("fsdp")
    chip, even = me // 2, me % 2 == 0
    side = lax.axis_index("dp") if paired else jnp.zeros((), jnp.int32)
    place = ring_place(chip, chips)
    heads = d // HEAD_DIM // 4
    width = heads * HEAD_DIM
    half = 3 * width
    tall = 2 * own_rows
    fold, packed = own_rows == HEAD_DIM, tall % 128 == 0
    plan = (chips, half, tall, fold, packed)
    starts = image_starts.shape[1]
    far = chips // 2

    proj_state = {1: [proj_weight], -1: [proj_weight]}
    if fold:
        with jax.named_scope("proj_gather"):
            gather_step(proj_state, chips, False)

    parts = qkv_weight.reshape(own_rows, 3, 2, heads, 2, HEAD_DIM).transpose(4, 0, 2, 1, 3, 5)
    parts = parts.reshape(2, own_rows, 2 * half)
    mine, others = jnp.where(even, parts[0], parts[1]), jnp.where(even, parts[1], parts[0])
    vec = jnp.stack([norm_gain, norm_shift])
    if packed:
        line = jnp.pad(vec.reshape(1, 2 * own_rows), ((0, 7), (0, 2 * half - 2 * own_rows)))
        others = jnp.concatenate([others, line], axis=0)
    got = swap_cores(others)
    got, line = got[:own_rows], got[own_rows:]
    block = jnp.where(
        even, jnp.concatenate([mine, got], axis=0), jnp.concatenate([got, mine], axis=0)
    )
    left, right = block[:, :half], block[:, half:]
    block_first = jnp.where(side == 0, left, right)
    block_second = jnp.where(side == 0, right, left)
    if packed:
        peer_vec = line[0, : 2 * own_rows].reshape(2, own_rows)
        pair = jnp.where(
            even, jnp.concatenate([vec, peer_vec], axis=1), jnp.concatenate([peer_vec, vec], axis=1)
        )
        line = jnp.pad(pair.reshape(1, 2 * tall), ((0, 7), (0, half - 2 * tall)))
        block_first = jnp.concatenate([block_first, line], axis=0)
    first_state = {1: [block_first], -1: [block_first]}
    for _ in range(far):
        with jax.named_scope("first_gather"):
            gather_step(first_state, chips, True)
        if fold:
            with jax.named_scope("proj_gather"):
                gather_step(proj_state, chips, False)
    pieces_first = gather_pieces(first_state)
    if paired:
        with jax.named_scope("hand_over"):
            handed = {
                (step, n): swap_bit(first_state[step][n], "dp", 1)
                for n in range(1, far + 1)
                for step in (1, -1)
                if n < len(first_state[step])
            }
        pieces_second = [block_second]
        for step in (1, -1):
            pieces_second += [handed[step, n] for n in range(1, len(first_state[step]))]
    else:
        second_state = {1: [block_second], -1: [block_second]}
        for _ in range(far):
            gather_step(second_state, chips, True)
        pieces_second = gather_pieces(second_state)

    meta = jnp.concatenate([patch_count, image_starts[0]])
    meta = jnp.concatenate([meta, swap_cores(meta)])

    def table(wide):
        offs = jnp.array(offsets(chips, wide), jnp.int32)
        return ring_chip((place + offs) % chips, chips).astype(jnp.int32)

    at_q, at_p = table(True), table(False)
    flag = side.astype(jnp.int32).reshape(1)
    two = 2 * rows
    normed, cots = call(
        functools.partial(norm_kernel, starts), "norm", [],
        [((two, d), f32), ((two, d), bf16)], two * d * 20,
        meta, tokens, swap_cores(tokens), cotangent, swap_cores(cotangent),
    )
    if fold:
        slabs = gather_pieces(proj_state)
    else:
        proj = lax.all_gather(proj_weight, "fsdp", axis=0, tiled=True)
        proj = proj.reshape(2 * heads, 2, HEAD_DIM, d)
        slabs = [jnp.where(even, proj[:, 0], proj[:, 1]).reshape(2 * width, d)]
    extra = []
    if not packed:
        whole = jnp.zeros((2, owners, own_rows), bf16)
        whole = lax.dynamic_update_slice(whole, vec[:, None], (0, me, 0))
        extra = [small_sum(whole.reshape(2, d), ("fsdp",))]
    projected = [((d, half), bf16), ((two, half), bf16), ((two, width), bf16)]
    work = two * d * 2

    def attend(qkv, grads):
        return call(
            functools.partial(attend_kernel, rows, starts, heads), "attend", [],
            [((two, width), bf16), ((two, half), bf16)], two * rows * heads * HEAD_DIM * 48,
            meta, qkv, grads,
        )

    with jax.named_scope("project_first"):
        weight_first, qkv_first, grads_first, hid, proj, gains = call(
            functools.partial(project_first_kernel, plan), "project", [],
            projected + [((two, d), bf16), ((2 * width, d), bf16), ((2, d), f32)],
            work * (half + width),
            at_q, at_p, flag, normed, cots, *pieces_first, *slabs, *extra,
        )
    with jax.named_scope("attend_first"):
        att_first, grad_first = attend(qkv_first, grads_first)
    index = {o: i for i, o in enumerate(offsets(chips, True))}
    if paired:
        order = [[index[o] for o in (-n, n - 1) if o in index] for n in range(far, 0, -1)]
    else:
        order = [[j] for j in range(chips)]
    with jax.named_scope("terms_first"):
        terms_first = call(
            functools.partial(terms_first_kernel, plan, order), "terms", [((d, half), bf16)],
            [((tall * len(js), half), bf16) for js in order], work * half,
            at_q, hid, grad_first,
        )
    given = {}
    if paired:
        with jax.named_scope("hand_back"):
            for js, term in zip(order, terms_first):
                back = swap_bit(term, "dp", 1)
                for i, j in enumerate(js):
                    given[j] = back[i * tall : (i + 1) * tall]

    with jax.named_scope("project_second"):
        weight_second, qkv_second, grads_second = call(
            functools.partial(project_second_kernel, plan), "project", [], projected,
            work * (half + width), at_q, flag, hid, cots, proj, *pieces_second,
        )
    with jax.named_scope("attend_second"):
        att_second, grad_second = attend(qkv_second, grads_second)
    proj_shape = ((2 * width, d), bf16)
    with jax.named_scope("terms_second"):
        terms_second = call(
            functools.partial(terms_second_kernel, plan), "terms",
            [((d, half), bf16)] + ([proj_shape] if fold else []),
            [((tall, half), bf16)] * chips
            + ([((HEAD_DIM, d), bf16)] * chips if fold else [proj_shape]),
            work * (half + width),
            at_q, at_p, flag, hid, grad_second, cots, att_first, att_second,
        )
    terms_q, terms_p = terms_second[:chips], terms_second[chips:]
    at = {o: [terms_q[i]] + ([given[i]] if paired else []) for o, i in index.items()}
    scatter_q = Scatter(at, chips, True)
    rings = [scatter_q]
    if fold:
        at = {o: [terms_p[i]] for i, o in enumerate(offsets(chips, False))}
        scatter_p = Scatter(at, chips, False)
        rings.append(scatter_p)
    if not paired:
        at = {o: [terms_first[i]] for i, o in enumerate(offsets(chips, True))}
        scatter_first = Scatter(at, chips, True)
        rings.append(scatter_first)
    for ring in rings:
        ring.step()
    with jax.named_scope("hidden"):
        own, peer = call(
            hidden_kernel, "hidden", [], [((rows, d), f32), ((rows, d), bf16)],
            work * half * 2,
            after(grad_first, terms_q[0]), weight_first, grad_second, weight_second,
        )
    grad_block, vec_term = call(
        last_kernel, "last", [], [((rows, d), bf16), ((2, d), f32)], rows * d * 40,
        tokens, cotangent, gains, own, swap_cores(peer),
    )
    sum_q = scatter_q.done()

    scale = 1.0 / math.sqrt(rows * replicas * owners)

    def settle(total):
        low, high = total[:own_rows], total[own_rows:]
        return jnp.where(even, low, high), jnp.where(even, high, low)

    keep, give = settle(sum_q)
    if fold:
        o_sum = scatter_p.done()
    else:
        proj_term = terms_p[0].reshape(2 * heads, HEAD_DIM, d)
        none = jnp.zeros_like(proj_term)
        spread = jnp.stack(
            [jnp.where(even, proj_term, none), jnp.where(even, none, proj_term)], axis=1
        )
        o_sum = lax.psum_scatter(spread.reshape(d, d), "fsdp", scatter_dimension=0, tiled=True)
    if paired:
        proj_grad = (o_sum.astype(f32) + swap_bit(o_sum, "dp", 1).astype(f32)) * scale
        sums = (swap_bit(keep, "dp", 1), swap_replica_and_core(give), keep, swap_cores(give))
    else:
        proj_grad = lax.psum(o_sum, "dp").astype(f32) * scale
        keep, give = lax.psum(keep, "dp"), lax.psum(give, "dp")
        keep1, give1 = settle(scatter_first.done())
        keep1, give1 = lax.psum(keep1, "dp"), lax.psum(give1, "dp")
        sums = (keep1, swap_cores(give1), keep, swap_cores(give))
    flags = jnp.stack([(me % 2).astype(jnp.int32), side.astype(jnp.int32)])
    (qkv_grad,) = call(
        functools.partial(finish_kernel, heads, scale), "finish", [],
        [((own_rows, 4 * half), f32)], own_rows * half * 40, flags, *sums,
    )
    vec_sum = small_sum(vec_term, ("fsdp", "dp")) * scale
    vec_own = lax.dynamic_slice(vec_sum, (0, me * own_rows), (2, own_rows))
    return grad_block, qkv_grad, proj_grad, vec_own[0], vec_own[1]


def solution(mesh):
    both = P(("dp", "fsdp"))
    rows2 = P(("dp", "fsdp"), None)
    own2, own = P("fsdp", None), P("fsdp")
    return jax.shard_map(
        per_device,
        mesh=mesh,
        in_specs=(rows2, rows2, both, rows2, own2, own2, own, own),
        out_specs=(rows2, own2, own2, own, own),
        check_vma=False,
    )
```
